256 devices in a mesh: variant: 4 (over y), sub: 64 (over x, z, core).
Axes of the slice: x: 4, y: 4, z: 8, core: 2. Of those that a mesh axis runs over, the one named last changes fastest.
Arguments:
- displacement: float32 [4, 6, 8192], P('variant', None, 'sub'), may hold values from -6 to 6
- neighbours: int32 [2, 8192], P(None, 'sub'), may hold values from 0 to 129, as said below
- micro_state: bfloat16 [4, 196608, 512], P('variant', 'sub'), may hold values from -6 to 6
- strain_loads: float32 [4, 6, 512], P('variant'), may hold values from -3 to 3
- stiffness: bfloat16 [4, 512, 512], P('variant'), may hold values from -0.25 to 0.25
- expand_weight: bfloat16 [4, 512, 2048], P('variant'), may hold values from -0.25 to 0.25
- contract_weight: bfloat16 [4, 2048, 512], P('variant'), may hold values from -0.125 to 0.125
- batch_route: int32 [4, 2, 1536], P('variant', None, 'sub'), may hold values from -1 to 63, as said below
- yield_flags: int32 [4, 196608], P('variant', 'sub'), may hold values 0 or 1
- readout: bfloat16 [4, 512], P('variant'), may hold values from -0.75 to 0.75
- external_force: float32 [4, 8192], P('variant', 'sub'), may hold values from -6 to 6
- coarse_inverse: bfloat16 [4, 8192, 8192], P('variant', 'sub'), may hold values from -0.0625 to 0.0625
Outputs:
- states_next: bfloat16 [4, 196608, 512], P('variant', 'sub')
- coarse_correction: float32 [4, 8192], P('variant', 'sub')
The draws below stay inside these ranges and needn't reach their ends.
Inputs may be any that keep to these rules, and one draw needn't show every extreme that they name: `neighbours`: entry 0 is position i or i + 1 of macro point i within its device (i counted from 0 in the device), entry 1 is i + 1 or i + 2, and entry 1 exceeds entry 0; the first and last point of each device use i and i + 2. `batch_route`: entry 0 of a batch held by device s on sub is -1 or (s + d) % 64 for some d from 1 to 16, each d used by at most one batch of s; entry 1 is -1 where entry 0 is, else its slot there, 0 to 7. Batches sent to one device have different slots; every device receives at most 8 batches, and in every draw some device receives 8.
All inputs are finite; a program needn't handle non-finite values. No bound on the sum of `yield_flags` on one device may be relied on, other than what follows from the above.
Results may differ from the reference program's by a relative error of at most 0.0055.
Values may be sent and summed in bfloat16 or wider, within the bound.
A program may use at most 64 MiB of HBM per device.

```python
import jax
import jax.numpy as jnp
from jax import lax

MP_DEV = 128
RPP = 24
BATCH = 128
MODES = 512
HIDDEN_SIZE = 2048
STRAIN = 6
VARIANTS = 4
COARSE = 8192
ROWS = 196608
BAT_DEV = 24
SPREAD = 16
CAP = 8
N_SUB = 64


def draw_neighbours(key, part):
    key = jax.random.fold_in(key, 17)
    total = MP_DEV * N_SUB
    pattern = jax.random.randint(key, (total,), 0, 3)
    position = jnp.arange(total) % MP_DEV
    pattern = jnp.where((position == 0) | (position == MP_DEV - 1), 0, pattern)
    centre = position + 1
    lower_index = jnp.where(pattern == 2, centre, centre - 1)
    upper_index = jnp.where(pattern == 1, centre, centre + 1)
    return jnp.stack([lower_index, upper_index]).astype(jnp.int32)


def draw_batch_route(key, part):
    key = jax.random.fold_in(key, 29)

    def per_variant(variant_key):
        key_phase, key_full, key_shift, key_order, key_chance = jax.random.split(variant_key, 5)
        phase = jax.random.randint(key_phase, (), 0, SPREAD)
        full_target = jax.random.randint(key_full, (), 0, N_SUB)
        batch_shift = jax.random.randint(key_shift, (N_SUB,), 0, BAT_DEV)
        order = jax.random.permutation(key_order, BAT_DEV)[:SPREAD]
        chance = jax.random.randint(key_chance, (N_SUB, SPREAD), 0, 4)
        sender = jnp.arange(N_SUB)[:, None]
        step_ahead = jnp.arange(1, SPREAD + 1)[None, :]
        receiver = (sender + step_ahead) % N_SUB
        rank = (sender + phase) % SPREAD
        is_hot = rank < CAP
        alive = is_hot & ((chance < 3) | (receiver == full_target))
        batch_index = sender * BAT_DEV + (batch_shift[:, None] + order[None, :]) % BAT_DEV
        landing = jnp.where(alive, batch_index, N_SUB * BAT_DEV).reshape(-1)
        target_list = jnp.full((N_SUB * BAT_DEV,), -1, jnp.int32).at[landing].set(receiver.reshape(-1).astype(jnp.int32), mode='drop')
        slot_list = jnp.full((N_SUB * BAT_DEV,), -1, jnp.int32).at[landing].set(jnp.broadcast_to(rank, (N_SUB, SPREAD)).reshape(-1).astype(jnp.int32), mode='drop')
        return jnp.stack([target_list, slot_list])
    variant_keys = jax.random.split(key, VARIANTS)
    return jax.vmap(per_variant)(variant_keys).astype(jnp.int32)


def set_ends(values, own_key, least, top_value):
    longest = values.shape.index(max(values.shape))
    spots = []
    for shift in (0, 1):
        where = [jax.random.randint(jax.random.fold_in(own_key, axis), (), 0, length) for axis, length in enumerate(values.shape)]
        where[longest] = (where[longest] + shift) % values.shape[longest]
        spots.append(tuple(where))
    return values.at[spots[0]].set(least).at[spots[1]].set(top_value)


def block_levels(stream_key, shape, shards, least, high):
    level, own = 1.0, jax.random.fold_in(stream_key, 6)
    for dim, blocks in shards:
        draws = jnp.exp(jax.random.uniform(jax.random.fold_in(own, dim), (blocks,), jnp.float32, least / len(shards), high / len(shards)))
        level = level * jnp.repeat(draws, shape[dim] // blocks).reshape([-1 if axis == dim else 1 for axis in range(len(shape))])
    return level


def bell_draw(own_key, extent, width, most, cuts=(), held_as=jnp.bfloat16):
    loudness = block_levels(own_key, extent, cuts, -0.22, 0.18) if cuts else 1.0
    result = jax.random.normal(own_key, extent, jnp.float32) * width * loudness
    return jnp.minimum(jnp.maximum(result, -most), most).astype(held_as)


def setup_inputs(seed: int = 0) -> dict:
    splits = jax.random.split(jax.random.key(seed), 13)
    displacement = bell_draw(splits[0], (VARIANTS, STRAIN, COARSE), 1.0, 6.0, ((0, 4), (2, 64)), jnp.float32)
    neighbours = draw_neighbours(jax.random.fold_in(splits[12], 71), 0)
    micro_state = bell_draw(splits[2], (VARIANTS, ROWS, MODES), 1.0, 6.0, ((0, 4), (1, 64)))
    strain_loads = bell_draw(splits[3], (VARIANTS, STRAIN, MODES), 4 ** -0.5, 3.0, ((0, 4),), jnp.float32)
    stiffness = bell_draw(splits[4], (VARIANTS, MODES, MODES), MODES ** -0.5, 0.25, ((0, 4),))
    expand_weight = bell_draw(splits[5], (VARIANTS, MODES, HIDDEN_SIZE), MODES ** -0.5, 0.25, ((0, 4),))
    contract_weight = bell_draw(splits[6], (VARIANTS, HIDDEN_SIZE, MODES), HIDDEN_SIZE ** -0.5, 0.125, ((0, 4),))
    batch_route = draw_batch_route(jax.random.fold_in(splits[12], 71), 0)
    yield_flags = set_ends((jax.random.randint(splits[8], (VARIANTS, ROWS), 0, 2) < 1).astype(jnp.int32), jax.random.fold_in(splits[8], 1), 0, 1)
    readout = bell_draw(splits[9], (VARIANTS, MODES), (MODES // 8) ** -0.5, 0.75, ((0, 4),))
    external_force = bell_draw(splits[10], (VARIANTS, COARSE), 1.0, 6.0, ((0, 4), (1, 64)), jnp.float32)
    coarse_inverse = bell_draw(splits[11], (VARIANTS, COARSE, COARSE), COARSE ** -0.5, 0.0625, ((0, 4), (1, 64)))
    return {"displacement": displacement, "neighbours": neighbours, "micro_state": micro_state, "strain_loads": strain_loads, "stiffness": stiffness, "expand_weight": expand_weight, "contract_weight": contract_weight, "batch_route": batch_route, "yield_flags": yield_flags, "readout": readout, "external_force": external_force, "coarse_inverse": coarse_inverse}


def plastic_update(row_block, expand_weight, contract_weight):
    hidden = jax.nn.silu(jnp.dot(row_block, expand_weight, preferred_element_type=jnp.float32)).astype(jnp.bfloat16)
    return jnp.dot(hidden, contract_weight, preferred_element_type=jnp.float32).astype(jnp.bfloat16)


def reference(displacement, neighbours, micro_state, strain_loads, stiffness, expand_weight, contract_weight, batch_route, yield_flags, readout, external_force, coarse_inverse):
    points = displacement.shape[2]
    owner_base = (jnp.arange(points) // MP_DEV).astype(jnp.int32) * MP_DEV
    first_index = owner_base + neighbours[0].astype(jnp.int32)
    second_index = owner_base + neighbours[1].astype(jnp.int32)
    spacing = (neighbours[1] - neighbours[0]).astype(jnp.float32)
    batch_count = ROWS // BATCH
    slot_total = N_SUB * SPREAD
    sender = (jnp.arange(batch_count) // BAT_DEV).astype(jnp.int32)

    def variant_step(inputs):
        macro_field, state_rows, load_rows, stiff_matrix, w_up, w_down, route_rows, flag_rows, readout_vec, force_rows, inverse = inputs
        padded = jnp.pad(macro_field, ((0, 0), (1, 1)))
        strain = (padded[:, second_index] - padded[:, first_index]) / spacing
        per_row = jnp.repeat(strain, RPP, axis=1)
        trial_state = state_rows.astype(jnp.float32) + jnp.dot(per_row.T, load_rows, precision=lax.Precision.HIGHEST)
        elastic = jnp.dot(trial_state.astype(jnp.bfloat16), stiff_matrix, preferred_element_type=jnp.float32)
        elastic_half = elastic.astype(jnp.bfloat16)
        batches = elastic_half.reshape(batch_count, BATCH, MODES)
        target = route_rows[0].astype(jnp.int32)
        alive_batch = target >= 0
        offset = (target - sender) % N_SUB
        position = jnp.where(alive_batch, sender * SPREAD + offset - 1, slot_total).astype(jnp.int32)
        slot_table = jnp.full((slot_total,), batch_count, jnp.int32).at[position].set(jnp.arange(batch_count, dtype=jnp.int32), mode="drop")
        with_blank = jnp.concatenate([batches, jnp.zeros((1, BATCH, MODES), jnp.bfloat16)], axis=0)
        received = with_blank[slot_table]
        updated = lax.map(lambda block_rows: plastic_update(block_rows, w_up, w_down), received)
        handed_back = updated[jnp.minimum(position, slot_total - 1)]
        handed_back = jnp.where(alive_batch[:, None, None], handed_back, jnp.zeros_like(handed_back))
        correction = handed_back.reshape(ROWS, MODES).astype(jnp.float32)
        weight_rows = (jnp.repeat(alive_batch.astype(jnp.int32), BATCH) * flag_rows).astype(jnp.float32)
        next_state = (elastic + weight_rows[:, None] * correction).astype(jnp.bfloat16)
        projected = jnp.dot(next_state, readout_vec, preferred_element_type=jnp.float32)
        averaged = jnp.mean(projected.reshape(points, RPP), axis=1)
        residual = (force_rows - averaged).astype(jnp.bfloat16)
        coarse = jnp.dot(inverse, residual, preferred_element_type=jnp.float32)
        return next_state, coarse

    return lax.map(variant_step, (displacement, micro_state, strain_loads, stiffness, expand_weight, contract_weight, batch_route, yield_flags, readout, external_force, coarse_inverse))
```

```python
import functools

import jax
import jax.numpy as jnp
from jax import lax
from jax.experimental import pallas as pl
from jax.experimental.pallas import tpu as pltpu
from jax.sharding import PartitionSpec as P

BATCH = 128
RPP = 24
BATCHES = 24
POINTS = 128
ROWS = 3072
MODES = 512
HIDDEN = 2048
TILE = 384
TILES = ROWS // TILE
WINDOW = BATCH + 16
PACKED = 2048 + 256
F32, BF16, I32 = jnp.float32, jnp.bfloat16, jnp.int32
MESH = pl.DeviceIdType.MESH


def mm(a, b, dims=((1,), (0,)), precision=None):
    return lax.dot_general(a, b, (dims, ((), ())), precision=precision, preferred_element_type=F32)


def micro_kernel(
    route_ref, flags_ref, disp_ref, before_ref, after_ref, neigh_ref, loads_ref, readout_ref, force_ref,
    micro_hbm, stiff_hbm, expand_hbm, contract_hbm,
    next_hbm, resid_ref,
    states, stiff, expand, contract, elastic, packed, update, delta, slot_t, sums, offs_v, offs_s,
    in_sem, w_sem, out_sem, offs_sem,
):
    def tile_rows(t):
        return pl.ds(t * TILE, TILE)

    loads_in = [pltpu.make_async_copy(micro_hbm.at[tile_rows(t)], states.at[tile_rows(t)], in_sem.at[t]) for t in range(TILES)]
    stiff_in = pltpu.make_async_copy(stiff_hbm, stiff, w_sem.at[0])
    expand_in = pltpu.make_async_copy(expand_hbm, expand, w_sem.at[1])
    contract_in = pltpu.make_async_copy(contract_hbm, contract, w_sem.at[2])
    stiff_in.start()
    for copy in loads_in:
        copy.start()
    expand_in.start()
    contract_in.start()

    sub_i = lax.broadcasted_iota(I32, (128, 128), 0)
    lane_i = lax.broadcasted_iota(I32, (128, 128), 1)
    before_mask = (sub_i < lane_i).astype(BF16)
    flags = jnp.concatenate(
        [flags_ref[0:1, b * BATCH:(b + 1) * BATCH] for b in range(BATCHES)] + [jnp.zeros((128 - BATCHES, 128), I32)], axis=0
    ).astype(F32)
    flags_b = flags.astype(BF16)
    offs_v[...] = jnp.full((8, 128), -1, I32)
    offs_v[1:2, 0:BATCHES] = route_ref[0:1, :]
    alive = (offs_v[1:2, :] >= 0).astype(F32)
    totals = mm(jnp.ones((8, 128), BF16), flags_b, ((1,), (1,))) * alive
    offsets = mm(totals.astype(BF16), before_mask)
    offs_v[0:1, :] = offsets[0:1, :].astype(I32)
    offs_v[1:2, :] = alive.astype(I32)
    offs_copy = pltpu.make_async_copy(offs_v, offs_s, offs_sem)
    offs_copy.start()
    slot = jnp.where(flags > 0, mm(flags_b, before_mask), -1.0e6)
    slot_t[...] = slot.T
    slot_i = slot.astype(I32)

    disp = disp_ref[...]
    lane6 = lax.broadcasted_iota(I32, (6, 128), 1)
    prev = jnp.where(lane6 == 0, before_ref[...], pltpu.roll(disp, 1, 1))
    follow = jnp.where(lane6 == POINTS - 1, after_ref[...], pltpu.roll(disp, POINTS - 1, 1))
    low_i, high_i = neigh_ref[0:1, :], neigh_ref[1:2, :]
    here = lax.broadcasted_iota(I32, (1, 128), 1)
    lower = jnp.where(low_i == here, prev, disp)
    upper = jnp.where(high_i == here + 2, follow, disp)
    strain = (upper - lower) / (high_i - low_i).astype(F32)
    strain_t = jnp.concatenate([strain, jnp.zeros((122, 128), F32)], axis=0).T
    total = strain_t[:, 0:1] * loads_ref[0:1, :]
    for k in range(1, 6):
        total = total + strain_t[:, k:k + 1] * loads_ref[k:k + 1, :]
    delta[...] = total

    packed[0:16, :] = jnp.zeros((16, MODES), BF16)
    row_w = lax.broadcasted_iota(I32, (WINDOW, 128), 0)
    stiff_in.wait()
    offs_copy.wait()
    for t in range(TILES):
        loads_in[t].wait()
        shift = jnp.concatenate(
            [jnp.broadcast_to(delta[p:p + 1, :], (RPP, MODES)) for p in range(t * 16, t * 16 + 16)], axis=0
        )
        trial = (states[tile_rows(t), :].astype(F32) + shift).astype(BF16)
        rows = mm(trial, stiff[...])
        elastic[tile_rows(t), :] = rows
        half = rows.astype(BF16)
        for j in range(3):
            b = t * 3 + j
            off, live = offs_s[0, b], offs_s[1, b]
            base = pl.multiple_of((off // 16) * 16, 16)
            lead = jnp.where(live > 0, off - base, -1000000)
            pick = (row_w == slot_i[b:b + 1, :] + lead).astype(BF16)
            got = mm(pick, half[j * BATCH:(j + 1) * BATCH, :]).astype(BF16)
            packed[pl.ds(base, 16), :] = packed[pl.ds(base, 16), :] + got[0:16]
            packed[pl.ds(base + 16, BATCH), :] = got[16:]

    expand_in.wait()
    contract_in.wait()
    count = offs_s[0, BATCHES]
    packed[pl.ds(pl.multiple_of(((count + 15) // 16) * 16, 16), BATCH), :] = jnp.zeros((BATCH, MODES), BF16)

    def plastic(start, length):
        x = packed[pl.ds(start, length), :]
        acc = None
        for n in range(4):
            a = mm(x, expand[:, n * 512:(n + 1) * 512])
            h = (a * (0.5 + 0.5 * jnp.tanh(0.5 * a))).astype(BF16)
            part = mm(h, contract[n * 512:(n + 1) * 512, :])
            acc = part if acc is None else acc + part
        update[pl.ds(start, length), :] = acc.astype(BF16)

    whole = (count + 127) // 256

    @pl.loop(0, whole)
    def _(i):
        plastic(pl.multiple_of(i * 256, 256), 256)

    done = pl.multiple_of(whole * 256, 256)

    @pl.when(count > done)
    def _():
        plastic(done, 128)

    tail = pl.multiple_of(((count + 127) // 128) * 128, 128)
    update[pl.ds(tail, WINDOW), :] = jnp.zeros((WINDOW, MODES), BF16)

    lane_w = lax.broadcasted_iota(I32, (BATCH, WINDOW), 1).astype(F32)
    members = (
        lax.broadcasted_iota(I32, (16, TILE), 1) // RPP == lax.broadcasted_iota(I32, (16, TILE), 0)
    ).astype(BF16)
    copies_out = []
    for t in range(TILES):
        for j in range(3):
            b = t * 3 + j
            off, live = offs_s[0, b], offs_s[1, b]
            base = pl.multiple_of((off // 16) * 16, 16)
            lead = jnp.where(live > 0, off - base, -1000000).astype(F32)
            put = (slot_t[:, b:b + 1] + lead == lane_w).astype(BF16)
            back = mm(put, update[pl.ds(base, WINDOW), :])
            rows = pl.ds(b * BATCH, BATCH)
            states[rows, :] = (elastic[rows, :] + back).astype(BF16)
        copy = pltpu.make_async_copy(states.at[tile_rows(t)], next_hbm.at[tile_rows(t)], out_sem.at[t])
        copy.start()
        copies_out.append(copy)
        sums[t * 16:(t + 1) * 16, :] = mm(members, states[tile_rows(t), :])
    weighed = sums[...] * readout_ref[...].astype(F32)
    lanes = weighed[:, 0:128] + weighed[:, 128:256] + weighed[:, 256:384] + weighed[:, 384:512]
    mean = jnp.sum(lanes.T, axis=0, keepdims=True) / RPP
    resid_ref[...] = (force_ref[...] - mean).astype(BF16).astype(F32)
    for copy in copies_out:
        copy.wait()


def micro_step(route, flags, disp, before, after, neigh, loads, readout, force, micro, stiff, expand, contract):
    vmem = pl.BlockSpec(memory_space=pltpu.VMEM)
    hbm = pl.BlockSpec(memory_space=pl.ANY)
    return pl.pallas_call(
        micro_kernel,
        name="micro",
        out_shape=(jax.ShapeDtypeStruct((ROWS, MODES), BF16), jax.ShapeDtypeStruct((1, POINTS), F32)),
        in_specs=[vmem] * 9 + [hbm] * 4,
        out_specs=(hbm, vmem),
        scratch_shapes=[
            pltpu.VMEM((ROWS, MODES), BF16),
            pltpu.VMEM((MODES, MODES), BF16),
            pltpu.VMEM((MODES, HIDDEN), BF16),
            pltpu.VMEM((HIDDEN, MODES), BF16),
            pltpu.VMEM((ROWS, MODES), F32),
            pltpu.VMEM((PACKED, MODES), BF16),
            pltpu.VMEM((PACKED, MODES), BF16),
            pltpu.VMEM((POINTS, MODES), F32),
            pltpu.VMEM((128, 128), F32),
            pltpu.VMEM((POINTS, MODES), F32),
            pltpu.VMEM((8, 128), I32),
            pltpu.SMEM((8, 128), I32),
            pltpu.SemaphoreType.DMA((TILES,)),
            pltpu.SemaphoreType.DMA((3,)),
            pltpu.SemaphoreType.DMA((TILES,)),
            pltpu.SemaphoreType.DMA,
        ],
        cost_estimate=pl.CostEstimate(flops=10_000_000_000, bytes_accessed=11_000_000, transcendentals=2_000_000),
    )(route, flags, disp, before, after, neigh, loads, readout, force, micro, stiff, expand, contract)


def coarse_kernel(devices, resid_ref, inverse_hbm, out_ref, inverse, blocks, in_sem, send_sem, recv_sem):
    me = lax.axis_index("sub")
    load = pltpu.make_async_copy(inverse_hbm, inverse, in_sem)
    load.start()
    barrier = pltpu.get_barrier_semaphore()
    for d in range(1, devices):
        pl.semaphore_signal(barrier, inc=1, device_id={"sub": lax.rem(me + d, devices)}, device_id_type=MESH)
    pl.semaphore_wait(barrier, devices - 1)
    sends = []
    for d in range(1, devices):
        copy = pltpu.make_async_remote_copy(
            src_ref=resid_ref,
            dst_ref=blocks.at[me],
            send_sem=send_sem,
            recv_sem=recv_sem,
            device_id={"sub": lax.rem(me + d, devices)},
            device_id_type=MESH,
        )
        copy.start()
        sends.append(copy)
    blocks[me] = resid_ref[...]
    load.wait()
    everyone = blocks.at[pl.ds(0, devices - 1)]
    pltpu.make_async_copy(everyone, everyone, recv_sem).wait()
    acc = None
    for s in range(devices):
        part = inverse[:, s * POINTS:(s + 1) * POINTS].astype(F32) * blocks[s]
        acc = part if acc is None else acc + part
    out_ref[...] = jnp.sum(acc.T, axis=0, keepdims=True)
    pltpu.make_async_copy(everyone, everyone, send_sem).wait()


def coarse_step(resid, inverse, devices):
    return pl.pallas_call(
        functools.partial(coarse_kernel, devices),
        name="coarse",
        out_shape=jax.ShapeDtypeStruct((1, POINTS), F32),
        in_specs=[pl.BlockSpec(memory_space=pltpu.VMEM), pl.BlockSpec(memory_space=pl.ANY)],
        out_specs=pl.BlockSpec(memory_space=pltpu.VMEM),
        scratch_shapes=[
            pltpu.VMEM(inverse.shape, BF16),
            pltpu.VMEM((devices, 1, POINTS), F32),
            pltpu.SemaphoreType.DMA,
            pltpu.SemaphoreType.DMA,
            pltpu.SemaphoreType.DMA,
        ],
        compiler_params=pltpu.CompilerParams(collective_id=0, has_side_effects=True),
        cost_estimate=pl.CostEstimate(flops=2_000_000, bytes_accessed=2_100_000, transcendentals=0),
    )(resid, inverse)


def on_device(
    displacement, neighbours, micro_state, strain_loads, stiffness, expand_weight, contract_weight,
    batch_route, yield_flags, readout, external_force, coarse_inverse,
):
    devices = lax.axis_size("sub")
    disp = displacement[0]
    up = [(i, i + 1) for i in range(devices - 1)]
    down = [(i + 1, i) for i in range(devices - 1)]
    before = lax.ppermute(disp[:, POINTS - 1:], "sub", up)
    after = lax.ppermute(disp[:, :1], "sub", down)
    next_state, resid = micro_step(
        batch_route[0], yield_flags, disp, before, after, neighbours, strain_loads[0], readout, external_force,
        micro_state[0], stiffness[0], expand_weight[0], contract_weight[0],
    )
    coarse = coarse_step(resid, coarse_inverse[0], devices)
    return next_state[None], coarse


def solution(mesh):
    return jax.shard_map(
        on_device,
        mesh=mesh,
        in_specs=(
            P("variant", None, "sub"),
            P(None, "sub"),
            P("variant", "sub", None),
            P("variant", None, None),
            P("variant", None, None),
            P("variant", None, None),
            P("variant", None, None),
            P("variant", None, "sub"),
            P("variant", "sub"),
            P("variant", None),
            P("variant", "sub"),
            P("variant", "sub", None),
        ),
        out_specs=(P("variant", "sub", None), P("variant", "sub")),
        check_vma=False,
    )
```

```python
import functools

import jax
import jax.numpy as jnp
from jax import lax
from jax.experimental import pallas as pl
from jax.experimental.pallas import tpu as pltpu
from jax.sharding import PartitionSpec as P

BATCH = 128
RPP = 24
BATCHES = 24
SLOTS = 16
POINTS = 128
ROWS = 3072
MODES = 512
HIDDEN = 2048
STRAIN = 6
TILE = 384
TILES = ROWS // TILE
F32, BF16, I32 = jnp.float32, jnp.bfloat16, jnp.int32
MESH = pl.DeviceIdType.MESH


def mm(a, b, dims=((1,), (0,))):
    return lax.dot_general(a, b, (dims, ((), ())), preferred_element_type=F32)


def row_tile(rows):
    return jnp.concatenate(rows + [jnp.zeros((128 - len(rows), 128), rows[0].dtype)], axis=0)


def newton_kernel(
    devices,
    route_ref, flags_ref, disp_ref, neigh_ref, loads_ref, readout_ref, force_ref,
    micro_hbm, stiff_hbm, expand_hbm, contract_hbm, inverse_hbm,
    next_ref, coarse_ref,
    states, stiff, expand, contract, inverse, elastic, hidden, update, delta, weight_t, sums, halo, resid, blocks,
    in_sem, w_sem, halo_send, halo_recv, send_sem, recv_sem,
):
    def tile_rows(t):
        return pl.ds(t * TILE, TILE)

    me = lax.axis_index("sub") if devices > 1 else 0
    micro_in = [pltpu.make_async_copy(micro_hbm.at[tile_rows(t)], states.at[tile_rows(t)], in_sem.at[t]) for t in range(TILES)]
    stiff_in = pltpu.make_async_copy(stiff_hbm, stiff, w_sem.at[0])
    expand_in = pltpu.make_async_copy(expand_hbm, expand, w_sem.at[1])
    contract_in = pltpu.make_async_copy(contract_hbm, contract, w_sem.at[2])
    inverse_in = pltpu.make_async_copy(inverse_hbm, inverse, w_sem.at[3])
    stiff_in.start()
    for copy in micro_in:
        copy.start()
    expand_in.start()
    contract_in.start()
    inverse_in.start()
    if devices > 1:
        barrier = pltpu.get_barrier_semaphore()
        for d in range(1, devices):
            pl.semaphore_signal(barrier, inc=1, device_id={"sub": lax.rem(me + d, devices)}, device_id_type=MESH)

    alive = [(route_ref[0, b] >= 0).astype(I32) for b in range(BATCHES)]
    ranks, upto, seen = [], [], jnp.int32(0)
    for b in range(1, BATCHES - 1):
        ranks.append(seen)
        seen = seen + alive[b]
        upto.append(seen)

    def inner(rank):
        passed = jnp.int32(1)
        for total in upto:
            passed = passed + (total <= rank).astype(I32)
        return jnp.minimum(passed, BATCHES - 2)

    first, last = alive[0] > 0, alive[-1] > 0
    held = [inner(j) for j in range(SLOTS)]
    held[15] = jnp.where(last, BATCHES - 1, jnp.where(first, held[14], held[15]))
    held[14] = jnp.where(first, 0, held[14])
    slots = [jnp.int32(14)] + [
        jnp.minimum(jnp.where(rank == 14, jnp.where(first, 15, 14), rank), SLOTS - 1) for rank in ranks
    ] + [jnp.int32(15)]

    weight_t[...] = row_tile([flags_ref[0:1, b * BATCH:(b + 1) * BATCH] for b in range(BATCHES)]).astype(F32).T

    here = lax.broadcasted_iota(I32, (1, POINTS), 1)
    low_i, high_i = neigh_ref[0:1, :], neigh_ref[1:2, :]
    spacing = (high_i - low_i).astype(F32)

    def shift_of(before, after):
        rows = []
        for k in range(STRAIN):
            disp = disp_ref[k]
            prev = jnp.where(here == 0, before(k), pltpu.roll(disp, 1, 1))
            follow = jnp.where(here == POINTS - 1, after(k), pltpu.roll(disp, POINTS - 1, 1))
            lower = jnp.where(low_i == here, prev, disp)
            upper = jnp.where(high_i == here + 2, follow, disp)
            rows.append((upper - lower) / spacing)
        return row_tile(rows).T

    def load_of(strain_t, part):
        total = strain_t[part, 0:1] * loads_ref[0]
        for k in range(1, STRAIN):
            total = total + strain_t[part, k:k + 1] * loads_ref[k]
        return total

    delta[...] = load_of(shift_of(lambda k: 0.0, lambda k: 0.0), slice(0, POINTS))

    def elastic_of(t, batches):
        shift = jnp.concatenate(
            [jnp.broadcast_to(delta[p:p + 1, :], (RPP, MODES)) for p in range(t * 16, t * 16 + 16)], axis=0
        )
        lo, hi = batches[0] * BATCH - t * TILE, (batches[-1] + 1) * BATCH - t * TILE
        trial = (states[tile_rows(t), :][lo:hi].astype(F32) + shift[lo:hi]).astype(BF16)
        rows = mm(trial, stiff[...]).astype(BF16)
        for j, b in enumerate(batches):
            elastic[b] = rows[j * BATCH:(j + 1) * BATCH]

    stiff_in.wait()
    for t in range(TILES):
        micro_in[t].wait()
        elastic_of(t, [b for b in range(t * 3, t * 3 + 3) if 0 < b < BATCHES - 1])

    def plastic(group):
        x = jnp.concatenate([elastic[held[j]] for j in group], axis=0)
        length = len(group) * BATCH
        for n in range(4):
            cols = slice(n * 512, (n + 1) * 512)
            a = mm(x, expand[:, cols])
            hidden[0:length, cols] = (a * (0.5 + 0.5 * jnp.tanh(0.5 * a))).astype(BF16)
        out = mm(hidden[0:length, :], contract[...]).astype(BF16)
        for i, j in enumerate(group):
            update[j] = out[i * BATCH:(i + 1) * BATCH]

    expand_in.wait()
    contract_in.wait()
    plastic([0, 1, 2, 3])
    plastic([4, 5, 6, 7])
    halo_copies = []
    if devices > 1:
        pl.semaphore_wait(barrier, devices - 1)
        for side, step in ((0, 1), (1, devices - 1)):
            copy = pltpu.make_async_remote_copy(
                src_ref=disp_ref, dst_ref=halo.at[side], send_sem=halo_send.at[side], recv_sem=halo_recv.at[side],
                device_id={"sub": lax.rem(me + step, devices)}, device_id_type=MESH,
            )
            copy.start()
            halo_copies.append(copy)
    plastic([8, 9, 10, 11])
    for copy in halo_copies:
        copy.wait()

    def before(k):
        return jnp.where(me == 0, 0.0, pltpu.roll(halo[0, k], 1, 1))

    def after(k):
        return jnp.where(me == devices - 1, 0.0, pltpu.roll(halo[1, k], POINTS - 1, 1))

    strain_t = shift_of(before, after)
    delta[0:8, :] = load_of(strain_t, slice(0, 8))
    delta[POINTS - 8:, :] = load_of(strain_t, slice(POINTS - 8, POINTS))
    elastic_of(0, [0])
    elastic_of(TILES - 1, [BATCHES - 1])
    plastic([12, 13, 14, 15])

    members = (
        lax.broadcasted_iota(I32, (16, TILE), 1) // RPP == lax.broadcasted_iota(I32, (16, TILE), 0)
    ).astype(BF16)
    for t in range(TILES):
        for b in range(t * 3, t * 3 + 3):
            weight = weight_t[:, b:b + 1] * alive[b].astype(F32)
            rows = elastic[b].astype(F32) + weight * update[slots[b]].astype(F32)
            next_ref[b * BATCH:(b + 1) * BATCH, :] = rows.astype(BF16)
        sums[t * 16:(t + 1) * 16, :] = mm(members, next_ref[tile_rows(t), :])
    weighed = sums[...] * readout_ref[...].astype(F32)
    lanes = weighed[:, 0:128] + weighed[:, 128:256] + weighed[:, 256:384] + weighed[:, 384:512]
    mean = jnp.sum(lanes.T, axis=0, keepdims=True) / RPP
    resid[...] = (force_ref[...] - mean).astype(BF16).astype(F32)

    inverse_in.wait()
    if devices == 1:
        coarse_ref[...] = resid[...]
        return
    for d in range(1, devices):
        pltpu.make_async_remote_copy(
            src_ref=resid, dst_ref=blocks.at[me], send_sem=send_sem, recv_sem=recv_sem,
            device_id={"sub": lax.rem(me + d, devices)}, device_id_type=MESH,
        ).start()
    blocks[me] = resid[...]
    others = blocks.at[pl.ds(0, devices - 1)]
    pltpu.make_async_copy(others, others, recv_sem).wait()
    acc = None
    for s in range(devices):
        part = inverse[:, s * POINTS:(s + 1) * POINTS].astype(F32) * blocks[s]
        acc = part if acc is None else acc + part
    coarse_ref[...] = jnp.sum(acc.T, axis=0, keepdims=True)
    pltpu.make_async_copy(others, others, send_sem).wait()


def newton_step(devices, *operands):
    smem = pl.BlockSpec(memory_space=pltpu.SMEM)
    vmem = pl.BlockSpec(memory_space=pltpu.VMEM)
    hbm = pl.BlockSpec(memory_space=pl.ANY)
    params = pltpu.CompilerParams(collective_id=0, has_side_effects=True) if devices > 1 else None
    return pl.pallas_call(
        functools.partial(newton_kernel, devices),
        name="newton",
        out_shape=(jax.ShapeDtypeStruct((ROWS, MODES), BF16), jax.ShapeDtypeStruct((1, POINTS), F32)),
        in_specs=[smem] + [vmem] * 6 + [hbm] * 5,
        out_specs=(vmem, vmem),
        scratch_shapes=[
            pltpu.VMEM((ROWS, MODES), BF16),
            pltpu.VMEM((MODES, MODES), BF16),
            pltpu.VMEM((MODES, HIDDEN), BF16),
            pltpu.VMEM((HIDDEN, MODES), BF16),
            pltpu.VMEM((POINTS, 64 * POINTS), BF16),
            pltpu.VMEM((BATCHES, BATCH, MODES), BF16),
            pltpu.VMEM((4 * BATCH, HIDDEN), BF16),
            pltpu.VMEM((SLOTS, BATCH, MODES), BF16),
            pltpu.VMEM((POINTS, MODES), F32),
            pltpu.VMEM((128, 128), F32),
            pltpu.VMEM((POINTS, MODES), F32),
            pltpu.VMEM((2, STRAIN, 1, POINTS), F32),
            pltpu.VMEM((1, POINTS), F32),
            pltpu.VMEM((64, 1, POINTS), F32),
            pltpu.SemaphoreType.DMA((TILES,)),
            pltpu.SemaphoreType.DMA((4,)),
            pltpu.SemaphoreType.DMA((2,)),
            pltpu.SemaphoreType.DMA((2,)),
            pltpu.SemaphoreType.DMA,
            pltpu.SemaphoreType.DMA,
        ],
        compiler_params=params,
    )(*operands)


def on_device(
    displacement, neighbours, micro_state, strain_loads, stiffness, expand_weight, contract_weight,
    batch_route, yield_flags, readout, external_force, coarse_inverse,
):
    next_state, coarse = newton_step(
        lax.axis_size("sub"),
        batch_route[0], yield_flags, displacement.transpose(1, 0, 2), neighbours, strain_loads.transpose(1, 0, 2),
        readout, external_force, micro_state[0], stiffness[0], expand_weight[0], contract_weight[0], coarse_inverse[0],
    )
    return next_state[None], coarse


def solution(mesh):
    return jax.shard_map(
        on_device,
        mesh=mesh,
        in_specs=(
            P("variant", None, "sub"),
            P(None, "sub"),
            P("variant", "sub", None),
            P("variant", None, None),
            P("variant", None, None),
            P("variant", None, None),
            P("variant", None, None),
            P("variant", None, "sub"),
            P("variant", "sub"),
            P("variant", None),
            P("variant", "sub"),
            P("variant", "sub", None),
        ),
        out_specs=(P("variant", "sub", None), P("variant", "sub")),
        check_vma=False,
    )
```

```python
import functools

import jax
import jax.numpy as jnp
from jax import lax
from jax.experimental import pallas as pl
from jax.experimental.pallas import tpu as pltpu
from jax.sharding import PartitionSpec as P

BATCH = 128
RPP = 24
BATCHES = 24
LIMIT = 58 << 20
PIECE = 32
SLOTS = 16
POINTS = 128
ROWS = 3072
MODES = 512
HIDDEN = 2048
STRAIN = 6
TILE = 384
TILES = ROWS // TILE
F32, BF16, I32 = jnp.float32, jnp.bfloat16, jnp.int32
MESH = pl.DeviceIdType.MESH


def mm(a, b, dims=((1,), (0,))):
    return lax.dot_general(a, b, (dims, ((), ())), preferred_element_type=F32)


def row_tile(rows):
    return jnp.concatenate(rows + [jnp.zeros((128 - len(rows), 128), rows[0].dtype)], axis=0)


def newton_kernel(
    devices,
    route_hbm, flags_hbm, disp_hbm, neigh_hbm, loads_hbm, readout_hbm, force_hbm,
    micro_hbm, stiff_hbm, expand_hbm, contract_hbm, inverse_hbm,
    next_ref, coarse_ref,
    route_ref, flags_ref, disp_ref, neigh_ref, loads_ref, readout_ref, force_ref,
    states, stiff, expand, contract, inverse, elastic, hidden, update, delta, weight_t, sums, halo, resid, blocks,
    small_sem, in_sem, w_sem, halo_send, halo_recv, send_sem, recv_sem,
):
    def tile_rows(t):
        return pl.ds(t * TILE, TILE)

    me = lax.axis_index("sub") if devices > 1 else 0
    micro_in = [pltpu.make_async_copy(micro_hbm.at[tile_rows(t)], states.at[tile_rows(t)], in_sem.at[t]) for t in range(TILES)]
    stiff_in = pltpu.make_async_copy(stiff_hbm, stiff, w_sem.at[0])
    expand_in = pltpu.make_async_copy(expand_hbm, expand, w_sem.at[1])
    contract_in = pltpu.make_async_copy(contract_hbm, contract, w_sem.at[2])
    inverse_in = pltpu.make_async_copy(inverse_hbm, inverse, w_sem.at[3])
    small_in = [
        pltpu.make_async_copy(src, dst, small_sem.at[i])
        for i, (src, dst) in enumerate((
            (disp_hbm, disp_ref), (neigh_hbm, neigh_ref), (loads_hbm, loads_ref),
            (route_hbm, route_ref), (flags_hbm, flags_ref), (readout_hbm, readout_ref), (force_hbm, force_ref),
        ))
    ]
    for copy in small_in[:3]:
        copy.start()
    stiff_in.start()
    for copy in micro_in[:2]:
        copy.start()
    for copy in small_in[3:]:
        copy.start()
    for copy in micro_in[2:]:
        copy.start()
    if devices > 1:
        barrier = pltpu.get_barrier_semaphore()
        for d in range(1, devices):
            pl.semaphore_signal(barrier, inc=1, device_id={"sub": lax.rem(me + d, devices)}, device_id_type=MESH)

    for copy in small_in[:3]:
        copy.wait()
    here = lax.broadcasted_iota(I32, (1, POINTS), 1)
    low_i, high_i = neigh_ref[0:1, :], neigh_ref[1:2, :]
    spacing = (high_i - low_i).astype(F32)

    def shift_of(before, after):
        rows = []
        for k in range(STRAIN):
            disp = disp_ref[k]
            prev = jnp.where(here == 0, before(k), pltpu.roll(disp, 1, 1))
            follow = jnp.where(here == POINTS - 1, after(k), pltpu.roll(disp, POINTS - 1, 1))
            lower = jnp.where(low_i == here, prev, disp)
            upper = jnp.where(high_i == here + 2, follow, disp)
            rows.append((upper - lower) / spacing)
        return row_tile(rows).T

    def load_of(strain_t, part):
        total = strain_t[part, 0:1] * loads_ref[0]
        for k in range(1, STRAIN):
            total = total + strain_t[part, k:k + 1] * loads_ref[k]
        return total

    delta[...] = load_of(shift_of(lambda k: 0.0, lambda k: 0.0), slice(0, POINTS))

    def elastic_of(t, batches):
        shift = jnp.concatenate(
            [jnp.broadcast_to(delta[p:p + 1, :], (RPP, MODES)) for p in range(t * 16, t * 16 + 16)], axis=0
        )
        lo, hi = batches[0] * BATCH - t * TILE, (batches[-1] + 1) * BATCH - t * TILE
        trial = (states[tile_rows(t), :][lo:hi].astype(F32) + shift[lo:hi]).astype(BF16)
        rows = mm(trial, stiff[...]).astype(BF16)
        for j, b in enumerate(batches):
            elastic[b] = rows[j * BATCH:(j + 1) * BATCH]

    def elastic_tile(t):
        micro_in[t].wait()
        elastic_of(t, [b for b in range(t * 3, t * 3 + 3) if 0 < b < BATCHES - 1])

    stiff_in.wait()
    for t in range(3):
        elastic_tile(t)
    expand_in.start()
    contract_in.start()
    for copy in small_in[3:]:
        copy.wait()
    alive = [(route_ref[0, b] >= 0).astype(I32) for b in range(BATCHES)]
    ranks, upto, seen = [], [], jnp.int32(0)
    for b in range(1, BATCHES - 1):
        ranks.append(seen)
        seen = seen + alive[b]
        upto.append(seen)

    def inner(rank):
        passed = jnp.int32(1)
        for total in upto:
            passed = passed + (total <= rank).astype(I32)
        return jnp.minimum(passed, BATCHES - 2)

    first, last = alive[0] > 0, alive[-1] > 0
    held = [inner(j) for j in range(SLOTS)]
    held[15] = jnp.where(last, BATCHES - 1, jnp.where(first, held[14], held[15]))
    held[14] = jnp.where(first, 0, held[14])
    slots = [jnp.int32(14)] + [
        jnp.minimum(jnp.where(rank == 14, jnp.where(first, 15, 14), rank), SLOTS - 1) for rank in ranks
    ] + [jnp.int32(15)]

    weight_t[...] = row_tile(
        [(flags_ref[0:1, b * BATCH:(b + 1) * BATCH] * alive[b]).astype(F32) for b in range(BATCHES)]
    ).T

    for t in range(3, TILES):
        elastic_tile(t)
    inverse_in.start()

    def plastic(group, between=()):
        x = jnp.concatenate([elastic[held[j]] for j in group], axis=0)
        length = len(group) * BATCH
        for n in range(4):
            cols = slice(n * 512, (n + 1) * 512)
            a = mm(x, expand[:, cols])
            hidden[0:length, cols] = (a * (0.5 + 0.5 * jnp.tanh(0.5 * a))).astype(BF16)
            if n < len(between):
                between[n]()
        out = mm(hidden[0:length, :], contract[...]).astype(BF16)
        for i, j in enumerate(group):
            update[j] = out[i * BATCH:(i + 1) * BATCH]

    members = (
        lax.broadcasted_iota(I32, (16, TILE), 1) // RPP == lax.broadcasted_iota(I32, (16, TILE), 0)
    ).astype(BF16)

    def finish(b):
        for r in range(0, BATCH, PIECE):
            part = slice(r, r + PIECE)
            rows = elastic[b, part].astype(F32) + weight_t[part, b:b + 1] * update[slots[b], part].astype(F32)
            next_ref[b * BATCH + r:b * BATCH + r + PIECE, :] = rows.astype(BF16)

    def sum_up(t):
        sums[t * 16:(t + 1) * 16, :] = mm(members, next_ref[tile_rows(t), :])

    expand_in.wait()
    contract_in.wait()
    plastic([0, 1, 2, 3])
    plastic([4, 5, 6, 7], [functools.partial(finish, b) for b in (1, 2, 3, 4)])
    halo_copies = []
    if devices > 1:
        pl.semaphore_wait(barrier, devices - 1)
        for side, step in ((0, 1), (1, devices - 1)):
            copy = pltpu.make_async_remote_copy(
                src_ref=disp_ref, dst_ref=halo.at[side], send_sem=halo_send.at[side], recv_sem=halo_recv.at[side],
                device_id={"sub": lax.rem(me + step, devices)}, device_id_type=MESH,
            )
            copy.start()
            halo_copies.append(copy)
    plastic([8, 9, 10, 11], [functools.partial(finish, b) for b in (5, 6, 7, 8)])
    for copy in halo_copies:
        copy.wait()

    def before(k):
        return jnp.where(me == 0, 0.0, pltpu.roll(halo[0, k], 1, 1))

    def after(k):
        return jnp.where(me == devices - 1, 0.0, pltpu.roll(halo[1, k], POINTS - 1, 1))

    strain_t = shift_of(before, after)
    delta[0:8, :] = load_of(strain_t, slice(0, 8))
    delta[POINTS - 8:, :] = load_of(strain_t, slice(POINTS - 8, POINTS))
    elastic_of(0, [0])
    elastic_of(TILES - 1, [BATCHES - 1])
    plastic([12, 13, 14, 15], [functools.partial(finish, b) for b in (9, 10, 11, 12)])
    for t in (1, 2, 3):
        sum_up(t)
    for t in (4, 5, 6, 7, 0):
        for b in range(t * 3, t * 3 + 3):
            if not 0 < b < 13:
                finish(b)
        sum_up(t)
    weighed = sums[...] * readout_ref[...].astype(F32)
    lanes = weighed[:, 0:128] + weighed[:, 128:256] + weighed[:, 256:384] + weighed[:, 384:512]
    mean = jnp.sum(lanes.T, axis=0, keepdims=True) / RPP
    resid[...] = (force_ref[...] - mean).astype(BF16).astype(F32)

    inverse_in.wait()
    if devices == 1:
        coarse_ref[...] = resid[...]
        return
    blocks[me] = resid[...]
    plane, depth, core = me // 16, lax.rem(me // 2, 8), lax.rem(me, 2)
    for dx, dz, dc in sorted(
        ((dx, dz, dc) for dx in range(4) for dz in range(8) for dc in range(2) if dx or dz or dc),
        key=lambda step: -min(step[0], 4 - step[0]) - min(step[1], 8 - step[1]),
    ):
        peer = lax.rem(plane + dx, 4) * 16 + lax.rem(depth + dz, 8) * 2 + lax.rem(core + dc, 2)
        pltpu.make_async_remote_copy(
            src_ref=resid, dst_ref=blocks.at[me], send_sem=send_sem, recv_sem=recv_sem.at[plane],
            device_id={"sub": peer}, device_id_type=MESH,
        ).start()
    acc = None
    for dx in (0, 1, 3, 2):
        near = lax.rem(plane + dx, 4)
        arrived = blocks.at[pl.ds(0, 15 if dx == 0 else 16)]
        pltpu.make_async_copy(arrived, arrived, recv_sem.at[near]).wait()
        for s in range(16):
            column = pl.multiple_of((near * 16 + s) * POINTS, POINTS)
            part = inverse[:, pl.ds(column, POINTS)].astype(F32) * blocks[near * 16 + s]
            acc = part if acc is None else acc + part
    coarse_ref[...] = jnp.sum(acc.T, axis=0, keepdims=True)
    others = blocks.at[pl.ds(0, devices - 1)]
    pltpu.make_async_copy(others, others, send_sem).wait()


def write_kernel(next_vmem, coarse_vmem, next_hbm, coarse_hbm, sem):
    part = ROWS // 4
    copies = [pltpu.make_async_copy(coarse_vmem, coarse_hbm, sem.at[4])]
    for i in range(4):
        rows = pl.ds(i * part, part)
        copies.append(pltpu.make_async_copy(next_vmem.at[rows], next_hbm.at[rows], sem.at[i]))
    for copy in copies:
        copy.start()
    for copy in copies:
        copy.wait()


def write_out(next_state, coarse):
    place = pl.BlockSpec(memory_space=pl.ANY)
    return pl.pallas_call(
        write_kernel,
        name="write",
        out_shape=(pltpu.HBM((ROWS, MODES), BF16), pltpu.HBM((1, POINTS), F32)),
        in_specs=[pl.BlockSpec(memory_space=pltpu.VMEM)] * 2,
        out_specs=(pl.BlockSpec(memory_space=pltpu.HBM),) * 2,
        scratch_shapes=[pltpu.SemaphoreType.DMA((5,))],
        compiler_params=pltpu.CompilerParams(vmem_limit_bytes=1 << 20),
    )(next_state, coarse)


def newton_step(devices, *operands):
    vmem = pl.BlockSpec(memory_space=pltpu.VMEM)
    hbm = pl.BlockSpec(memory_space=pltpu.HBM)
    params = (
        pltpu.CompilerParams(collective_id=0, has_side_effects=True, vmem_limit_bytes=LIMIT)
        if devices > 1
        else pltpu.CompilerParams(vmem_limit_bytes=LIMIT)
    )
    return pl.pallas_call(
        functools.partial(newton_kernel, devices),
        name="newton",
        out_shape=(pltpu.VMEM((ROWS, MODES), BF16), pltpu.VMEM((1, POINTS), F32)),
        in_specs=[hbm] * 12,
        out_specs=(vmem, vmem),
        scratch_shapes=[
            pltpu.SMEM((2, BATCHES), I32),
            pltpu.VMEM((1, ROWS), I32),
            pltpu.VMEM((STRAIN, 1, POINTS), F32),
            pltpu.VMEM((2, POINTS), I32),
            pltpu.VMEM((STRAIN, 1, MODES), F32),
            pltpu.VMEM((1, MODES), BF16),
            pltpu.VMEM((1, POINTS), F32),
            pltpu.VMEM((ROWS, MODES), BF16),
            pltpu.VMEM((MODES, MODES), BF16),
            pltpu.VMEM((MODES, HIDDEN), BF16),
            pltpu.VMEM((HIDDEN, MODES), BF16),
            pltpu.VMEM((POINTS, 64 * POINTS), BF16),
            pltpu.VMEM((BATCHES, BATCH, MODES), BF16),
            pltpu.VMEM((4 * BATCH, HIDDEN), BF16),
            pltpu.VMEM((SLOTS, BATCH, MODES), BF16),
            pltpu.VMEM((POINTS, MODES), F32),
            pltpu.VMEM((128, 128), F32),
            pltpu.VMEM((POINTS, MODES), F32),
            pltpu.VMEM((2, STRAIN, 1, POINTS), F32),
            pltpu.VMEM((1, POINTS), F32),
            pltpu.VMEM((64, 1, POINTS), F32),
            pltpu.SemaphoreType.DMA((7,)),
            pltpu.SemaphoreType.DMA((TILES,)),
            pltpu.SemaphoreType.DMA((4,)),
            pltpu.SemaphoreType.DMA((2,)),
            pltpu.SemaphoreType.DMA((2,)),
            pltpu.SemaphoreType.DMA,
            pltpu.SemaphoreType.DMA((4,)),
        ],
        compiler_params=params,
    )(*operands)


def on_device(
    displacement, neighbours, micro_state, strain_loads, stiffness, expand_weight, contract_weight,
    batch_route, yield_flags, readout, external_force, coarse_inverse,
):
    next_state, coarse = newton_step(
        lax.axis_size("sub"),
        batch_route[0], yield_flags, displacement.transpose(1, 0, 2), neighbours, strain_loads.transpose(1, 0, 2),
        readout, external_force, micro_state[0], stiffness[0], expand_weight[0], contract_weight[0], coarse_inverse[0],
    )
    next_state, coarse = write_out(next_state, coarse)
    return next_state[None], coarse


def solution(mesh):
    return jax.shard_map(
        on_device,
        mesh=mesh,
        in_specs=(
            P("variant", None, "sub"),
            P(None, "sub"),
            P("variant", "sub", None),
            P("variant", None, None),
            P("variant", None, None),
            P("variant", None, None),
            P("variant", None, None),
            P("variant", None, "sub"),
            P("variant", "sub"),
            P("variant", None),
            P("variant", "sub"),
            P("variant", "sub", None),
        ),
        out_specs=(P("variant", "sub", None), P("variant", "sub")),
        check_vma=False,
    )
```

```python
import functools

import jax
import jax.numpy as jnp
from jax import lax
from jax.experimental import pallas as pl
from jax.experimental.pallas import tpu as pltpu
from jax.sharding import PartitionSpec as P

BATCH = 128
RPP = 24
BATCHES = 24
LIMIT = 58 << 20
RB = 512
NB = 512
SLOTS = 16
POINTS = 128
ROWS = 3072
MODES = 512
HIDDEN = 2048
STRAIN = 6
TILE = 384
TILES = ROWS // TILE
F32, BF16, I32 = jnp.float32, jnp.bfloat16, jnp.int32
MESH = pl.DeviceIdType.MESH


def mm(a, b, dims=((1,), (0,))):
    return lax.dot_general(a, b, (dims, ((), ())), preferred_element_type=F32)


def row_tile(rows):
    return jnp.concatenate(rows + [jnp.zeros((128 - len(rows), 128), rows[0].dtype)], axis=0)


def newton_kernel(
    devices,
    route_hbm, flags_hbm, disp_hbm, neigh_hbm, loads_hbm, readout_hbm, force_hbm,
    micro_hbm, stiff_hbm, expand_hbm, contract_hbm, inverse_hbm,
    next_ref, coarse_ref,
    route_ref, flags_ref, disp_ref, neigh_ref, loads_ref, readout_ref, force_ref,
    states, stiff, expand, contract, inverse, elastic, hidden, update, delta, weight_t, sums, halo, resid, blocks,
    small_sem, in_sem, w_sem, halo_send, halo_recv, send_sem, recv_sem,
):
    def tile_rows(t):
        return pl.ds(t * TILE, TILE)

    me = lax.axis_index("sub") if devices > 1 else 0
    micro_in = [pltpu.make_async_copy(micro_hbm.at[tile_rows(t)], states.at[tile_rows(t)], in_sem.at[t]) for t in range(TILES)]
    stiff_in = pltpu.make_async_copy(stiff_hbm, stiff, w_sem.at[0])
    expand_in = pltpu.make_async_copy(expand_hbm, expand, w_sem.at[1])
    contract_in = pltpu.make_async_copy(contract_hbm, contract, w_sem.at[2])
    inverse_in = pltpu.make_async_copy(inverse_hbm, inverse, w_sem.at[3])
    small_in = [
        pltpu.make_async_copy(src, dst, small_sem.at[i])
        for i, (src, dst) in enumerate((
            (disp_hbm, disp_ref), (neigh_hbm, neigh_ref), (loads_hbm, loads_ref),
            (route_hbm, route_ref), (flags_hbm, flags_ref), (readout_hbm, readout_ref), (force_hbm, force_ref),
        ))
    ]
    for copy in small_in[:3]:
        copy.start()
    stiff_in.start()
    for copy in micro_in[:2]:
        copy.start()
    for copy in small_in[3:]:
        copy.start()
    for copy in micro_in[2:]:
        copy.start()
    expand_in.start()
    contract_in.start()
    if devices > 1:
        barrier = pltpu.get_barrier_semaphore()
        for d in range(1, devices):
            pl.semaphore_signal(barrier, inc=1, device_id={"sub": lax.rem(me + d, devices)}, device_id_type=MESH)

    for copy in small_in[:3]:
        copy.wait()
    here = lax.broadcasted_iota(I32, (1, POINTS), 1)
    low_i, high_i = neigh_ref[0:1, :], neigh_ref[1:2, :]
    spacing = (high_i - low_i).astype(F32)

    def shift_of(before, after):
        rows = []
        for k in range(STRAIN):
            disp = disp_ref[k]
            prev = jnp.where(here == 0, before(k), pltpu.roll(disp, 1, 1))
            follow = jnp.where(here == POINTS - 1, after(k), pltpu.roll(disp, POINTS - 1, 1))
            lower = jnp.where(low_i == here, prev, disp)
            upper = jnp.where(high_i == here + 2, follow, disp)
            rows.append((upper - lower) / spacing)
        return row_tile(rows).T

    def load_of(strain_t, part):
        total = strain_t[part, 0:1] * loads_ref[0]
        for k in range(1, STRAIN):
            total = total + strain_t[part, k:k + 1] * loads_ref[k]
        return total

    delta[...] = load_of(shift_of(lambda k: 0.0, lambda k: 0.0), slice(0, POINTS))

    def elastic_of(t, batches):
        shift = jnp.concatenate(
            [jnp.broadcast_to(delta[p:p + 1, :], (RPP, MODES)) for p in range(t * 16, t * 16 + 16)], axis=0
        )
        lo, hi = batches[0] * BATCH - t * TILE, (batches[-1] + 1) * BATCH - t * TILE
        trial = (states[tile_rows(t), :][lo:hi].astype(F32) + shift[lo:hi]).astype(BF16)
        rows = mm(trial, stiff[...]).astype(BF16)
        for j, b in enumerate(batches):
            elastic[b] = rows[j * BATCH:(j + 1) * BATCH]

    def elastic_tile(t, wait=True):
        if wait:
            micro_in[t].wait()
        elastic_of(t, [b for b in range(t * 3, t * 3 + 3) if 0 < b < BATCHES - 1])

    stiff_in.wait()
    for t in range(2):
        elastic_tile(t)
    for t in range(2, TILES):
        micro_in[t].wait()
    for copy in small_in[3:]:
        copy.wait()
    alive = [(route_ref[0, b] >= 0).astype(I32) for b in range(BATCHES)]
    ranks, upto, seen = [], [], jnp.int32(0)
    for b in range(1, BATCHES - 1):
        ranks.append(seen)
        seen = seen + alive[b]
        upto.append(seen)

    def inner(rank):
        passed = jnp.int32(1 + rank)
        for total in upto[rank:]:
            passed = passed + (total <= rank).astype(I32)
        return jnp.minimum(passed, BATCHES - 2)

    first, last = alive[0] > 0, alive[-1] > 0
    held = [inner(j) for j in range(SLOTS)]
    held[15] = jnp.where(last, BATCHES - 1, jnp.where(first, held[14], held[15]))
    held[14] = jnp.where(first, 0, held[14])
    slots = [jnp.int32(14)] + [
        jnp.minimum(jnp.where(rank == 14, jnp.where(first, 15, 14), rank), SLOTS - 1) for rank in ranks
    ] + [jnp.int32(15)]

    weight_t[...] = row_tile(
        [(flags_ref[0:1, b * BATCH:(b + 1) * BATCH] * alive[b]).astype(F32) for b in range(BATCHES)]
    ).T

    for t in range(2, TILES):
        elastic_tile(t, False)
    inverse_in.start()

    def plastic(group, between=()):
        x = jnp.concatenate([elastic[held[j]] for j in group], axis=0)
        length = len(group) * BATCH
        for n in range(HIDDEN // NB):
            cols = slice(n * NB, (n + 1) * NB)
            for r in range(0, length, RB):
                a = mm(x[r:r + RB], expand[:, cols])
                hidden[r:r + RB, cols] = (a * (0.5 + 0.5 * jnp.tanh(0.5 * a))).astype(BF16)
            for piece in between[n * NB // 512:(n + 1) * NB // 512]:
                piece()
        for r in range(0, length, RB):
            out = mm(hidden[r:r + RB, :], contract[...]).astype(BF16)
            for i in range(RB // BATCH):
                update[group[r // BATCH + i]] = out[i * BATCH:(i + 1) * BATCH]

    members = (
        lax.broadcasted_iota(I32, (16, TILE), 1) // RPP == lax.broadcasted_iota(I32, (16, TILE), 0)
    ).astype(BF16)

    def finish(b):
        weight = jnp.broadcast_to(weight_t[:, b:b + 1], (BATCH, 128)).astype(BF16)
        for c in range(0, MODES, 128):
            rows = elastic[b, :, c:c + 128] + weight * update[slots[b], :, c:c + 128]
            next_ref[b * BATCH:(b + 1) * BATCH, c:c + 128] = rows

    def sum_up(t):
        sums[t * 16:(t + 1) * 16, :] = mm(members, next_ref[tile_rows(t), :])

    expand_in.wait()
    contract_in.wait()
    plastic([0, 1, 2, 3])
    plastic([4, 5, 6, 7], [functools.partial(finish, b) for b in (1, 2, 3, 4)])
    halo_copies = []
    if devices > 1:
        pl.semaphore_wait(barrier, devices - 1)
        for side, step in ((0, 1), (1, devices - 1)):
            copy = pltpu.make_async_remote_copy(
                src_ref=disp_ref, dst_ref=halo.at[side], send_sem=halo_send.at[side], recv_sem=halo_recv.at[side],
                device_id={"sub": lax.rem(me + step, devices)}, device_id_type=MESH,
            )
            copy.start()
            halo_copies.append(copy)
    plastic([8, 9, 10, 11], [functools.partial(finish, b) for b in (5, 6, 7, 8)])
    for copy in halo_copies:
        copy.wait()

    def before(k):
        return jnp.where(me == 0, 0.0, pltpu.roll(halo[0, k], 1, 1))

    def after(k):
        return jnp.where(me == devices - 1, 0.0, pltpu.roll(halo[1, k], POINTS - 1, 1))

    strain_t = shift_of(before, after)
    delta[0:8, :] = load_of(strain_t, slice(0, 8))
    delta[POINTS - 8:, :] = load_of(strain_t, slice(POINTS - 8, POINTS))
    elastic_of(0, [0])
    elastic_of(TILES - 1, [BATCHES - 1])
    plastic([12, 13, 14, 15], [functools.partial(finish, b) for b in (9, 10, 11, 12)])
    for t in (1, 2, 3):
        sum_up(t)
    for t in (4, 5, 6, 7, 0):
        for b in range(t * 3, t * 3 + 3):
            if not 0 < b < 13:
                finish(b)
        sum_up(t)
    weighed = sums[...] * readout_ref[...].astype(F32)
    lanes = weighed[:, 0:128] + weighed[:, 128:256] + weighed[:, 256:384] + weighed[:, 384:512]
    mean = jnp.sum(lanes.T, axis=0, keepdims=True) / RPP
    resid[...] = (force_ref[...] - mean).astype(BF16).astype(F32)

    inverse_in.wait()
    if devices == 1:
        coarse_ref[...] = resid[...]
        return
    blocks[me] = resid[...]
    plane, depth, core = me // 16, lax.rem(me // 2, 8), lax.rem(me, 2)
    for dx, dz, dc in sorted(
        ((dx, dz, dc) for dx in range(4) for dz in range(8) for dc in range(2) if dx or dz or dc),
        key=lambda step: -min(step[0], 4 - step[0]) - min(step[1], 8 - step[1]),
    ):
        peer = lax.rem(plane + dx, 4) * 16 + lax.rem(depth + dz, 8) * 2 + lax.rem(core + dc, 2)
        pltpu.make_async_remote_copy(
            src_ref=resid, dst_ref=blocks.at[me], send_sem=send_sem, recv_sem=recv_sem.at[plane],
            device_id={"sub": peer}, device_id_type=MESH,
        ).start()
    acc = None
    for dx in (0, 1, 3, 2):
        near = lax.rem(plane + dx, 4)
        arrived = blocks.at[pl.ds(0, 15 if dx == 0 else 16)]
        pltpu.make_async_copy(arrived, arrived, recv_sem.at[near]).wait()
        for s in range(16):
            column = pl.multiple_of((near * 16 + s) * POINTS, POINTS)
            part = inverse[:, pl.ds(column, POINTS)].astype(F32) * blocks[near * 16 + s]
            acc = part if acc is None else acc + part
    coarse_ref[...] = jnp.sum(acc.T, axis=0, keepdims=True)
    others = blocks.at[pl.ds(0, devices - 1)]
    pltpu.make_async_copy(others, others, send_sem).wait()


def write_kernel(next_vmem, coarse_vmem, next_hbm, coarse_hbm, sem):
    part = ROWS // 4
    copies = [pltpu.make_async_copy(coarse_vmem, coarse_hbm, sem.at[4])]
    for i in range(4):
        rows = pl.ds(i * part, part)
        copies.append(pltpu.make_async_copy(next_vmem.at[rows], next_hbm.at[rows], sem.at[i]))
    for copy in copies:
        copy.start()
    for copy in copies:
        copy.wait()


def write_out(next_state, coarse):
    place = pl.BlockSpec(memory_space=pl.ANY)
    return pl.pallas_call(
        write_kernel,
        name="write",
        out_shape=(pltpu.HBM((ROWS, MODES), BF16), pltpu.HBM((1, POINTS), F32)),
        in_specs=[pl.BlockSpec(memory_space=pltpu.VMEM)] * 2,
        out_specs=(pl.BlockSpec(memory_space=pltpu.HBM),) * 2,
        scratch_shapes=[pltpu.SemaphoreType.DMA((5,))],
        compiler_params=pltpu.CompilerParams(vmem_limit_bytes=1 << 20),
    )(next_state, coarse)


def newton_step(devices, *operands):
    vmem = pl.BlockSpec(memory_space=pltpu.VMEM)
    hbm = pl.BlockSpec(memory_space=pltpu.HBM)
    params = (
        pltpu.CompilerParams(collective_id=0, has_side_effects=True, vmem_limit_bytes=LIMIT)
        if devices > 1
        else pltpu.CompilerParams(vmem_limit_bytes=LIMIT)
    )
    return pl.pallas_call(
        functools.partial(newton_kernel, devices),
        name="newton",
        out_shape=(pltpu.VMEM((ROWS, MODES), BF16), pltpu.VMEM((1, POINTS), F32)),
        in_specs=[hbm] * 12,
        out_specs=(vmem, vmem),
        scratch_shapes=[
            pltpu.SMEM((2, BATCHES), I32),
            pltpu.VMEM((1, ROWS), I32),
            pltpu.VMEM((STRAIN, 1, POINTS), F32),
            pltpu.VMEM((2, POINTS), I32),
            pltpu.VMEM((STRAIN, 1, MODES), F32),
            pltpu.VMEM((1, MODES), BF16),
            pltpu.VMEM((1, POINTS), F32),
            pltpu.VMEM((ROWS, MODES), BF16),
            pltpu.VMEM((MODES, MODES), BF16),
            pltpu.VMEM((MODES, HIDDEN), BF16),
            pltpu.VMEM((HIDDEN, MODES), BF16),
            pltpu.VMEM((POINTS, 64 * POINTS), BF16),
            pltpu.VMEM((BATCHES, BATCH, MODES), BF16),
            pltpu.VMEM((4 * BATCH, HIDDEN), BF16),
            pltpu.VMEM((SLOTS, BATCH, MODES), BF16),
            pltpu.VMEM((POINTS, MODES), F32),
            pltpu.VMEM((128, 128), F32),
            pltpu.VMEM((POINTS, MODES), F32),
            pltpu.VMEM((2, STRAIN, 1, POINTS), F32),
            pltpu.VMEM((1, POINTS), F32),
            pltpu.VMEM((64, 1, POINTS), F32),
            pltpu.SemaphoreType.DMA((7,)),
            pltpu.SemaphoreType.DMA((TILES,)),
            pltpu.SemaphoreType.DMA((4,)),
            pltpu.SemaphoreType.DMA((2,)),
            pltpu.SemaphoreType.DMA((2,)),
            pltpu.SemaphoreType.DMA,
            pltpu.SemaphoreType.DMA((4,)),
        ],
        compiler_params=params,
    )(*operands)


def on_device(
    displacement, neighbours, micro_state, strain_loads, stiffness, expand_weight, contract_weight,
    batch_route, yield_flags, readout, external_force, coarse_inverse,
):
    next_state, coarse = newton_step(
        lax.axis_size("sub"),
        batch_route[0], yield_flags, displacement.transpose(1, 0, 2), neighbours, strain_loads.transpose(1, 0, 2),
        readout, external_force, micro_state[0], stiffness[0], expand_weight[0], contract_weight[0], coarse_inverse[0],
    )
    next_state, coarse = write_out(next_state, coarse)
    return next_state[None], coarse


def solution(mesh):
    return jax.shard_map(
        on_device,
        mesh=mesh,
        in_specs=(
            P("variant", None, "sub"),
            P(None, "sub"),
            P("variant", "sub", None),
            P("variant", None, None),
            P("variant", None, None),
            P("variant", None, None),
            P("variant", None, None),
            P("variant", None, "sub"),
            P("variant", "sub"),
            P("variant", None),
            P("variant", "sub"),
            P("variant", "sub", None),
        ),
        out_specs=(P("variant", "sub", None), P("variant", "sub")),
        check_vma=False,
    )
```

```python
import functools

import jax
import jax.numpy as jnp
from jax import lax
from jax.experimental import pallas as pl
from jax.experimental.pallas import tpu as pltpu
from jax.sharding import PartitionSpec as P

BATCH = 128
RPP = 24
BATCHES = 24
LIMIT = 58 << 20
RB = 512
NB = 512
SLOTS = 16
POINTS = 128
ROWS = 3072
MODES = 512
HIDDEN = 2048
STRAIN = 6
TILE = 384
TILES = ROWS // TILE
F32, BF16, I32 = jnp.float32, jnp.bfloat16, jnp.int32
MESH = pl.DeviceIdType.MESH


def mm(a, b, dims=((1,), (0,))):
    return lax.dot_general(a, b, (dims, ((), ())), preferred_element_type=F32)


def row_tile(rows):
    return jnp.concatenate(rows + [jnp.zeros((128 - len(rows), 128), rows[0].dtype)], axis=0)


def newton_kernel(
    devices,
    route_hbm, flags_hbm, disp_hbm, neigh_hbm, loads_hbm, readout_hbm, force_hbm,
    micro_hbm, stiff_hbm, expand_hbm, contract_hbm, inverse_hbm,
    next_ref, coarse_ref,
    route_ref, flags_ref, disp_ref, neigh_ref, loads_ref, readout_ref, force_ref,
    states, stiff, expand, contract, inverse, elastic, hidden, update, delta, weight_t, sums, halo, resid, blocks,
    small_sem, in_sem, w_sem, halo_send, halo_recv, send_sem, recv_sem,
):
    def tile_rows(t):
        return pl.ds(t * TILE, TILE)

    me = lax.axis_index("sub") if devices > 1 else 0
    micro_in = [pltpu.make_async_copy(micro_hbm.at[tile_rows(t)], states.at[tile_rows(t)], in_sem.at[t]) for t in range(TILES)]
    stiff_in = pltpu.make_async_copy(stiff_hbm, stiff, w_sem.at[0])
    expand_in = pltpu.make_async_copy(expand_hbm, expand, w_sem.at[1])
    contract_in = pltpu.make_async_copy(contract_hbm, contract, w_sem.at[2])
    inverse_in = pltpu.make_async_copy(inverse_hbm, inverse, w_sem.at[3])
    small_in = [
        pltpu.make_async_copy(src, dst, small_sem.at[i])
        for i, (src, dst) in enumerate((
            (disp_hbm, disp_ref), (neigh_hbm, neigh_ref), (loads_hbm, loads_ref),
            (route_hbm, route_ref), (flags_hbm, flags_ref), (readout_hbm, readout_ref), (force_hbm, force_ref),
        ))
    ]
    for copy in small_in[:3]:
        copy.start()
    stiff_in.start()
    for copy in micro_in[:2]:
        copy.start()
    for copy in small_in[3:]:
        copy.start()
    for copy in micro_in[2:]:
        copy.start()
    expand_in.start()
    contract_in.start()
    if devices > 1:
        barrier = pltpu.get_barrier_semaphore()
        for d in range(1, devices):
            pl.semaphore_signal(barrier, inc=1, device_id={"sub": lax.rem(me + d, devices)}, device_id_type=MESH)

    for copy in small_in[:3]:
        copy.wait()
    here = lax.broadcasted_iota(I32, (1, POINTS), 1)
    low_i, high_i = neigh_ref[0:1, :], neigh_ref[1:2, :]
    spacing = (high_i - low_i).astype(F32)

    def shift_of(before, after):
        rows = []
        for k in range(STRAIN):
            disp = disp_ref[k]
            prev = jnp.where(here == 0, before(k), pltpu.roll(disp, 1, 1))
            follow = jnp.where(here == POINTS - 1, after(k), pltpu.roll(disp, POINTS - 1, 1))
            lower = jnp.where(low_i == here, prev, disp)
            upper = jnp.where(high_i == here + 2, follow, disp)
            rows.append((upper - lower) / spacing)
        return row_tile(rows).T

    def load_of(strain_t, part):
        total = strain_t[part, 0:1] * loads_ref[0]
        for k in range(1, STRAIN):
            total = total + strain_t[part, k:k + 1] * loads_ref[k]
        return total

    delta[...] = load_of(shift_of(lambda k: 0.0, lambda k: 0.0), slice(0, POINTS))

    def elastic_of(t, batches):
        shift = jnp.concatenate(
            [jnp.broadcast_to(delta[p:p + 1, :], (RPP, MODES)) for p in range(t * 16, t * 16 + 16)], axis=0
        )
        lo, hi = batches[0] * BATCH - t * TILE, (batches[-1] + 1) * BATCH - t * TILE
        trial = (states[tile_rows(t), :][lo:hi].astype(F32) + shift[lo:hi]).astype(BF16)
        rows = mm(trial, stiff[...]).astype(BF16)
        for j, b in enumerate(batches):
            elastic[b] = rows[j * BATCH:(j + 1) * BATCH]

    def elastic_tile(t, wait=True):
        if wait:
            micro_in[t].wait()
        elastic_of(t, [b for b in range(t * 3, t * 3 + 3) if 0 < b < BATCHES - 1])

    stiff_in.wait()
    for t in range(5):
        micro_in[t].wait()
    for t in range(5):
        elastic_tile(t, False)
    for t in range(5, TILES):
        micro_in[t].wait()
    for copy in small_in[3:]:
        copy.wait()
    alive = [(route_ref[0, b] >= 0).astype(I32) for b in range(BATCHES)]
    ranks, upto, seen = [], [], jnp.int32(0)
    for b in range(1, BATCHES - 1):
        ranks.append(seen)
        seen = seen + alive[b]
        upto.append(seen)

    def inner(rank):
        passed = jnp.int32(1 + rank)
        for total in upto[rank:]:
            passed = passed + (total <= rank).astype(I32)
        return jnp.minimum(passed, BATCHES - 2)

    first, last = alive[0] > 0, alive[-1] > 0
    held = [inner(j) for j in range(SLOTS)]
    held[15] = jnp.where(last, BATCHES - 1, jnp.where(first, held[14], held[15]))
    held[14] = jnp.where(first, 0, held[14])
    slots = [jnp.int32(14)] + [
        jnp.minimum(jnp.where(rank == 14, jnp.where(first, 15, 14), rank), SLOTS - 1) for rank in ranks
    ] + [jnp.int32(15)]

    weight_t[...] = row_tile(
        [(flags_ref[0:1, b * BATCH:(b + 1) * BATCH] * alive[b]).astype(F32) for b in range(BATCHES)]
    ).T

    for t in range(5, TILES):
        elastic_tile(t, False)
    inverse_in.start()

    def plastic(group, between=()):
        x = jnp.concatenate([elastic[held[j]] for j in group], axis=0)
        length = len(group) * BATCH
        for n in range(HIDDEN // NB):
            cols = slice(n * NB, (n + 1) * NB)
            for r in range(0, length, RB):
                a = mm(x[r:r + RB], expand[:, cols])
                hidden[r:r + RB, cols] = (a * (0.5 + 0.5 * jnp.tanh(0.5 * a))).astype(BF16)
            for piece in between[n * NB // 512:(n + 1) * NB // 512]:
                piece()
        for r in range(0, length, RB):
            out = mm(hidden[r:r + RB, :], contract[...]).astype(BF16)
            for i in range(RB // BATCH):
                update[group[r // BATCH + i]] = out[i * BATCH:(i + 1) * BATCH]

    members = (
        lax.broadcasted_iota(I32, (16, TILE), 1) // RPP == lax.broadcasted_iota(I32, (16, TILE), 0)
    ).astype(BF16)

    def finish(b):
        weight = jnp.broadcast_to(weight_t[:, b:b + 1], (BATCH, 128)).astype(BF16)
        for c in range(0, MODES, 128):
            rows = elastic[b, :, c:c + 128] + weight * update[slots[b], :, c:c + 128]
            next_ref[b * BATCH:(b + 1) * BATCH, c:c + 128] = rows

    def sum_up(t):
        sums[t * 16:(t + 1) * 16, :] = mm(members, next_ref[tile_rows(t), :])

    expand_in.wait()
    contract_in.wait()
    plastic([0, 1, 2, 3])
    plastic([4, 5, 6, 7], [functools.partial(finish, b) for b in (1, 2, 3, 4)])
    halo_copies = []
    if devices > 1:
        pl.semaphore_wait(barrier, devices - 1)
        for side, step in ((0, 1), (1, devices - 1)):
            copy = pltpu.make_async_remote_copy(
                src_ref=disp_ref, dst_ref=halo.at[side], send_sem=halo_send.at[side], recv_sem=halo_recv.at[side],
                device_id={"sub": lax.rem(me + step, devices)}, device_id_type=MESH,
            )
            copy.start()
            halo_copies.append(copy)
    plastic([8, 9, 10, 11], [functools.partial(finish, b) for b in (5, 6, 7, 8)])
    for copy in halo_copies:
        copy.wait()

    def before(k):
        return jnp.where(me == 0, 0.0, pltpu.roll(halo[0, k], 1, 1))

    def after(k):
        return jnp.where(me == devices - 1, 0.0, pltpu.roll(halo[1, k], POINTS - 1, 1))

    strain_t = shift_of(before, after)
    delta[0:8, :] = load_of(strain_t, slice(0, 8))
    delta[POINTS - 8:, :] = load_of(strain_t, slice(POINTS - 8, POINTS))
    elastic_of(0, [0])
    elastic_of(TILES - 1, [BATCHES - 1])
    plastic([12, 13, 14, 15], [functools.partial(finish, b) for b in (9, 10, 11, 12)])
    for t in (1, 2, 3):
        sum_up(t)
    for t in (4, 5, 6, 7, 0):
        for b in range(t * 3, t * 3 + 3):
            if not 0 < b < 13:
                finish(b)
        sum_up(t)
    weighed = sums[...] * readout_ref[...].astype(F32)
    lanes = weighed[:, 0:128] + weighed[:, 128:256] + weighed[:, 256:384] + weighed[:, 384:512]
    mean = jnp.sum(lanes.T, axis=0, keepdims=True) / RPP
    resid[...] = (force_ref[...] - mean).astype(BF16).astype(F32)

    inverse_in.wait()
    if devices == 1:
        coarse_ref[...] = resid[...]
        return
    blocks[me] = resid[...]
    plane, depth, core = me // 16, lax.rem(me // 2, 8), lax.rem(me, 2)
    for dx, dz, dc in sorted(
        ((dx, dz, dc) for dx in range(4) for dz in range(8) for dc in range(2) if dx or dz or dc),
        key=lambda step: -min(step[0], 4 - step[0]) - min(step[1], 8 - step[1]),
    ):
        peer = lax.rem(plane + dx, 4) * 16 + lax.rem(depth + dz, 8) * 2 + lax.rem(core + dc, 2)
        pltpu.make_async_remote_copy(
            src_ref=resid, dst_ref=blocks.at[me], send_sem=send_sem, recv_sem=recv_sem.at[plane],
            device_id={"sub": peer}, device_id_type=MESH,
        ).start()
    acc = None
    for dx in (0, 1, 3, 2):
        near = lax.rem(plane + dx, 4)
        arrived = blocks.at[pl.ds(0, 15 if dx == 0 else 16)]
        pltpu.make_async_copy(arrived, arrived, recv_sem.at[near]).wait()
        for s in range(16):
            column = pl.multiple_of((near * 16 + s) * POINTS, POINTS)
            part = inverse[:, pl.ds(column, POINTS)].astype(F32) * blocks[near * 16 + s]
            acc = part if acc is None else acc + part
    coarse_ref[...] = jnp.sum(acc.T, axis=0, keepdims=True)
    others = blocks.at[pl.ds(0, devices - 1)]
    pltpu.make_async_copy(others, others, send_sem).wait()


def write_kernel(next_vmem, coarse_vmem, next_hbm, coarse_hbm, sem):
    part = ROWS // 4
    copies = [pltpu.make_async_copy(coarse_vmem, coarse_hbm, sem.at[4])]
    for i in range(4):
        rows = pl.ds(i * part, part)
        copies.append(pltpu.make_async_copy(next_vmem.at[rows], next_hbm.at[rows], sem.at[i]))
    for copy in copies:
        copy.start()
    for copy in copies:
        copy.wait()


def write_out(next_state, coarse):
    place = pl.BlockSpec(memory_space=pl.ANY)
    return pl.pallas_call(
        write_kernel,
        name="write",
        out_shape=(pltpu.HBM((ROWS, MODES), BF16), pltpu.HBM((1, POINTS), F32)),
        in_specs=[pl.BlockSpec(memory_space=pltpu.VMEM)] * 2,
        out_specs=(pl.BlockSpec(memory_space=pltpu.HBM),) * 2,
        scratch_shapes=[pltpu.SemaphoreType.DMA((5,))],
        compiler_params=pltpu.CompilerParams(vmem_limit_bytes=1 << 20),
    )(next_state, coarse)


def newton_step(devices, *operands):
    vmem = pl.BlockSpec(memory_space=pltpu.VMEM)
    hbm = pl.BlockSpec(memory_space=pltpu.HBM)
    params = (
        pltpu.CompilerParams(collective_id=0, has_side_effects=True, vmem_limit_bytes=LIMIT)
        if devices > 1
        else pltpu.CompilerParams(vmem_limit_bytes=LIMIT)
    )
    return pl.pallas_call(
        functools.partial(newton_kernel, devices),
        name="newton",
        out_shape=(pltpu.VMEM((ROWS, MODES), BF16), pltpu.VMEM((1, POINTS), F32)),
        in_specs=[hbm] * 12,
        out_specs=(vmem, vmem),
        scratch_shapes=[
            pltpu.SMEM((2, BATCHES), I32),
            pltpu.VMEM((1, ROWS), I32),
            pltpu.VMEM((STRAIN, 1, POINTS), F32),
            pltpu.VMEM((2, POINTS), I32),
            pltpu.VMEM((STRAIN, 1, MODES), F32),
            pltpu.VMEM((1, MODES), BF16),
            pltpu.VMEM((1, POINTS), F32),
            pltpu.VMEM((ROWS, MODES), BF16),
            pltpu.VMEM((MODES, MODES), BF16),
            pltpu.VMEM((MODES, HIDDEN), BF16),
            pltpu.VMEM((HIDDEN, MODES), BF16),
            pltpu.VMEM((POINTS, 64 * POINTS), BF16),
            pltpu.VMEM((BATCHES, BATCH, MODES), BF16),
            pltpu.VMEM((4 * BATCH, HIDDEN), BF16),
            pltpu.VMEM((SLOTS, BATCH, MODES), BF16),
            pltpu.VMEM((POINTS, MODES), F32),
            pltpu.VMEM((128, 128), F32),
            pltpu.VMEM((POINTS, MODES), F32),
            pltpu.VMEM((2, STRAIN, 1, POINTS), F32),
            pltpu.VMEM((1, POINTS), F32),
            pltpu.VMEM((64, 1, POINTS), F32),
            pltpu.SemaphoreType.DMA((7,)),
            pltpu.SemaphoreType.DMA((TILES,)),
            pltpu.SemaphoreType.DMA((4,)),
            pltpu.SemaphoreType.DMA((2,)),
            pltpu.SemaphoreType.DMA((2,)),
            pltpu.SemaphoreType.DMA,
            pltpu.SemaphoreType.DMA((4,)),
        ],
        compiler_params=params,
    )(*operands)


def on_device(
    displacement, neighbours, micro_state, strain_loads, stiffness, expand_weight, contract_weight,
    batch_route, yield_flags, readout, external_force, coarse_inverse,
):
    next_state, coarse = newton_step(
        lax.axis_size("sub"),
        batch_route[0], yield_flags, displacement.transpose(1, 0, 2), neighbours, strain_loads.transpose(1, 0, 2),
        readout, external_force, micro_state[0], stiffness[0], expand_weight[0], contract_weight[0], coarse_inverse[0],
    )
    next_state, coarse = write_out(next_state, coarse)
    return next_state[None], coarse


def solution(mesh):
    return jax.shard_map(
        on_device,
        mesh=mesh,
        in_specs=(
            P("variant", None, "sub"),
            P(None, "sub"),
            P("variant", "sub", None),
            P("variant", None, None),
            P("variant", None, None),
            P("variant", None, None),
            P("variant", None, None),
            P("variant", None, "sub"),
            P("variant", "sub"),
            P("variant", None),
            P("variant", "sub"),
            P("variant", "sub", None),
        ),
        out_specs=(P("variant", "sub", None), P("variant", "sub")),
        check_vma=False,
    )
```
